32 devices in a mesh: dp: 16 (over z, x, core), head: 2 (over y).
Axes of the slice: x: 2, y: 2, z: 4, core: 2. Of those that a mesh axis runs over, the one named last changes fastest.
Arguments:
- layer_input: bfloat16 [16384, 768], P('dp', 'head'), may hold values from -6 to 6
- first_gain: float32 [768], replicated, may hold values from 0.5 to 1.5
- first_shift: float32 [768], replicated, may hold values from -3 to 3
- qkv_weight: bfloat16 [3, 768, 768], P(None, None, 'head'), may hold values from -0.5 to 0.5
- out_weight: bfloat16 [768, 768], P('head'), may hold values from -0.875 to 0.875
- second_gain: float32 [768], replicated, may hold values from 0.5 to 1.5
- second_shift: float32 [768], replicated, may hold values from -3 to 3
- up_weight: bfloat16 [768, 3072], P(None, 'head'), may hold values from -0.21875 to 0.21875
- down_weight: bfloat16 [3072, 768], P('head'), may hold values from -0.15625 to 0.15625
- segment_ids: int32 [16384], P('dp'), may hold values from 0 to 4, as said below
- pad_mask: int32 [16384], P('dp'), may hold values from 0 to 1, as said below
- cluster_ids: int32 [12, 16384], P('head', 'dp'), may hold values from 0 to 99, as said below
- output_grad: bfloat16 [16384, 768], P('dp', 'head'), may hold values from -6 to 6
Outputs:
- layer_output: bfloat16 [16384, 768], P('dp', 'head')
- input_grad: bfloat16 [16384, 768], P('dp', 'head')
- qkv_grad: float32 [3, 768, 768], P(None, None, 'head')
- mix_weight_grad: float32 [768, 768], P('head')
- up_grad: float32 [768, 3072], P(None, 'head')
- down_grad: float32 [3072, 768], P('head')
- first_gain_grad: float32 [768], replicated
- first_shift_grad: float32 [768], replicated
- second_gain_grad: float32 [768], replicated
- second_shift_grad: float32 [768], replicated
The draws below stay inside these ranges and needn't reach their ends.
Inputs may be any that keep to these rules, and one draw needn't show every extreme that they name: `segment_ids`: never falling within a sequence of 1024 tokens; 4 documents numbered 0 .. 3, each of 128 tokens or more, then one or more padding tokens numbered 4 at the sequence's end. `pad_mask`: 1 exactly on the tokens of documents, 0 on padding. `cluster_ids`: in each head and sequence every cluster holds at least one token with pad_mask 1, and all such tokens of a cluster lie in one document.
All inputs are finite; a program needn't handle non-finite values.
Results may differ from the reference program's by a relative error of at most 0.015.
The reference program's roundings to bfloat16 on the way count: a program that leaves them out, or rounds other values in their place, can miss the bound.
Values may be sent and summed in bfloat16 or wider, within the bound.
A program may use at most 128 MiB of HBM per device.

```python
import math
import jax
import jax.numpy as jnp
from jax import lax

D = 768
HEADS = 12
HDIM = 64
FF = 3072
CLUST = 100
DOCS = 4
TOK_DEV = 1024
TOKENS = 16384


def layout(key):
    base = jax.random.fold_in(key, 7)
    first_key, second_key = jax.random.split(base)
    seq_count = TOKENS // TOK_DEV
    padding = jax.random.randint(first_key, (seq_count,), 1, TOK_DEV // 8 + 1)
    filled = TOK_DEV - padding
    least = TOK_DEV // 8
    spare = filled - least * DOCS
    cuts = jax.random.randint(second_key, (seq_count, DOCS - 1), 0, spare[:, None] + 1)
    cuts = jnp.sort(cuts, axis=1)
    inner = cuts + least * jnp.arange(1, DOCS, dtype=jnp.int32)[None, :]
    starts = jnp.concatenate([jnp.zeros((seq_count, 1), jnp.int32), inner, filled[:, None]], axis=1)
    places = jnp.arange(TOK_DEV, dtype=jnp.int32)
    segment = jnp.sum((places[None, :, None] >= inner[:, None, :]).astype(jnp.int32), axis=-1)
    live = (places[None, :] < filled[:, None]).astype(jnp.int32)
    segment = jnp.where(live > 0, segment, DOCS)
    return (segment, live, starts, filled)


def draw_segment_ids(key, part):
    return layout(key)[0].reshape(TOKENS)


def draw_pad_mask(key, part):
    return layout(key)[1].reshape(TOKENS)


def draw_cluster_ids(key, part):
    segment, live, starts, filled = layout(key)
    seq_count = TOKENS // TOK_DEV
    places = jnp.arange(TOK_DEV, dtype=jnp.int32)
    bounds = CLUST * starts // filled[:, None]
    document = jnp.minimum(segment, DOCS - 1)
    low_bound = jnp.take_along_axis(bounds, document, axis=1)
    high_bound = jnp.take_along_axis(bounds, document + 1, axis=1)
    spread = high_bound - low_bound
    offset = places[None, :] - jnp.take_along_axis(starts, document, axis=1)
    head_key = jax.random.fold_in(key, 11)
    shift_key, pick_key, pad_key = jax.random.split(head_key, 3)
    shifts = jax.random.randint(shift_key, (HEADS, seq_count, DOCS), 0, TOK_DEV)
    wide_doc = jnp.broadcast_to(document[None], (HEADS, seq_count, TOK_DEV))
    doc_shift = jnp.take_along_axis(shifts, wide_doc, axis=2)
    covering = (offset[None] + doc_shift) % spread[None]
    picked = jax.random.randint(pick_key, (HEADS, seq_count, TOK_DEV), 0, spread[None])
    inside = jnp.where(offset[None] < spread[None], covering, picked) + low_bound[None]
    filler = jax.random.randint(pad_key, (HEADS, seq_count, TOK_DEV), 0, CLUST)
    labels = jnp.where(live[None] > 0, inside, filler)
    return labels.reshape(HEADS, TOKENS)


def level_of(rng, extent, shards, smallest, high):
    level = 1.0
    for position, blocks in shards:
        draws = jax.random.uniform(jax.random.fold_in(jax.random.fold_in(rng, 6), position), (blocks,), jnp.float32, smallest / len(shards), high / len(shards))
        level = level * jnp.repeat(jnp.exp(draws), extent[position] // blocks).reshape((-1,) + (1,) * (len(extent) - 1 - position))
    return level


def normal_values(stream_key, shape, scale, reach, cuts=(), kind=jnp.bfloat16):
    factor_of = level_of(stream_key, shape, cuts, -0.22, 0.18) if cuts else 1.0
    entries = jax.random.normal(stream_key, shape, jnp.float32) * scale * factor_of
    return jnp.minimum(jnp.maximum(entries, -reach), reach).astype(kind)


def setup_inputs(seed: int = 0) -> dict:
    streams_of = jax.random.split(jax.random.key(seed), 14)
    layer_input = normal_values(streams_of[0], (TOKENS, D), 1.0, 6.0, ((0, 16), (1, 2)))
    first_gain = jnp.clip(jax.random.uniform(streams_of[1], (D,), jnp.float32, 0.5, 1.5), 0.5, 1.5)
    first_shift = normal_values(streams_of[2], (D,), 0.5, 3.0, (), jnp.float32)
    qkv_weight = normal_values(streams_of[3], (3, D, D), 128 ** -0.5, 0.5, ((2, 2),))
    out_weight = normal_values(streams_of[4], (D, D), 48 ** -0.5, 0.875, ((0, 2),))
    second_gain = jnp.clip(jax.random.uniform(streams_of[5], (D,), jnp.float32, 0.5, 1.5), 0.5, 1.5)
    second_shift = normal_values(streams_of[6], (D,), 0.5, 3.0, (), jnp.float32)
    up_weight = normal_values(streams_of[7], (D, FF), D ** -0.5, 0.21875, ((1, 2),))
    down_weight = normal_values(streams_of[8], (FF, D), (FF // 2) ** -0.5, 0.15625, ((0, 2),))
    segment_ids = draw_segment_ids(jax.random.fold_in(streams_of[13], 71), 0)
    pad_mask = draw_pad_mask(jax.random.fold_in(streams_of[13], 71), 0)
    cluster_ids = draw_cluster_ids(jax.random.fold_in(streams_of[13], 71), 0)
    output_grad = normal_values(streams_of[12], (TOKENS, D), 1.0, 6.0, ((0, 16), (1, 2)))
    return {"layer_input": layer_input, "first_gain": first_gain, "first_shift": first_shift, "qkv_weight": qkv_weight, "out_weight": out_weight, "second_gain": second_gain, "second_shift": second_shift, "up_weight": up_weight, "down_weight": down_weight, "segment_ids": segment_ids, "pad_mask": pad_mask, "cluster_ids": cluster_ids, "output_grad": output_grad}


@jax.custom_vjp
def low(v):
    return lax.optimization_barrier(v.astype(jnp.bfloat16)).astype(jnp.float32)

@jax.custom_vjp
def low_back(v):
    return v

def low_keep(v):
    return (low(v), None)

def low_pass(kept, grad):
    return (grad,)

def back_keep(v):
    return (v, None)

def back_low(kept, grad):
    return (low(grad),)
low.defvjp(low_keep, low_pass)
low_back.defvjp(back_keep, back_low)
epsilon = 1e-05
far_below = -1e+30
highest = lax.Precision.HIGHEST

def normalize(values, gain, shift):
    row_mean = lax.optimization_barrier(jnp.mean(values, axis=-1, keepdims=True))
    centred = values - row_mean
    variance = lax.optimization_barrier(jnp.mean(centred * centred, axis=-1, keepdims=True))
    return centred * lax.rsqrt(variance + epsilon) * gain + shift

def clustered(query, keys, values, segment_ids, pad_mask, cluster_ids):
    live_rows = (pad_mask > 0).astype(jnp.float32)
    labels = jnp.arange(CLUST, dtype=jnp.int32)
    member = (cluster_ids[:, None, :] == labels[None, :, None]).astype(jnp.float32) * live_rows[None, None, :]
    counts = lax.optimization_barrier(jnp.sum(member, axis=-1))
    centre = low(jnp.einsum('hcs,she->hce', member, query, precision=highest) / counts[:, :, None])
    seg_float = segment_ids.astype(jnp.float32)
    doc_owner = jnp.einsum('hcs,s->hc', member, seg_float, precision=highest) / counts
    allowed = (jnp.abs(doc_owner[:, :, None] - seg_float[None, None, :]) < 0.5) & (pad_mask[None, None, :] > 0)
    scores = low_back(jnp.einsum('hce,she->hcs', centre, keys, precision=highest) * HDIM ** (-0.5))
    masked = jnp.where(allowed, scores, far_below)
    row_top = lax.optimization_barrier(jnp.max(masked, axis=-1, keepdims=True))
    expos = jnp.exp(masked - row_top)
    probs = low(expos / lax.optimization_barrier(jnp.sum(expos, axis=-1, keepdims=True)))
    centre_out = low_back(low(jnp.einsum('hcs,she->hce', probs, values, precision=highest)))
    return jnp.einsum('hcs,hce->she', member, centre_out, precision=highest)

def forward(layer_in, first_gain, first_shift, qkv_weight, out_weight, second_gain, second_shift, up_weight, down_weight, segment_ids, pad_mask, cluster_ids):
    groups, seq_len = (layer_in.shape[0], layer_in.shape[1])
    normed = low(normalize(layer_in, first_gain, first_shift))
    projected = low(low_back(jnp.einsum('gsd,ide->igse', normed, qkv_weight, precision=highest)))
    head_parts = projected.reshape(3, groups, seq_len, HEADS, HDIM)
    mixture = jax.vmap(clustered)(head_parts[0], head_parts[1], head_parts[2], segment_ids, pad_mask, cluster_ids)
    mixture = mixture.reshape(groups, seq_len, D)
    branch = low_back(jnp.einsum('gse,ed->gsd', mixture, out_weight, precision=highest))
    residual = layer_in + branch
    second = low(normalize(residual, second_gain, second_shift))
    hidden = low_back(jnp.einsum('gsd,df->gsf', second, up_weight, precision=highest))
    activated = low(jax.nn.gelu(hidden))
    return residual + low_back(jnp.einsum('gsf,fd->gsd', activated, down_weight, precision=highest))

def reference(layer_input, first_gain, first_shift, qkv_weight, out_weight, second_gain, second_shift, up_weight, down_weight, segment_ids, pad_mask, cluster_ids, output_grad):
    seq_count = TOKENS // TOK_DEV
    group = math.gcd(seq_count, max(1, 4096 // TOK_DEV))
    rounds = seq_count // group
    params = tuple((weight.astype(jnp.float32) for weight in (first_gain, first_shift, qkv_weight, out_weight, second_gain, second_shift, up_weight, down_weight)))
    inputs = layer_input.astype(jnp.float32).reshape(rounds, group, TOK_DEV, D)
    cotangents = output_grad.astype(jnp.float32).reshape(rounds, group, TOK_DEV, D)
    segments = segment_ids.reshape(rounds, group, TOK_DEV)
    masks = pad_mask.reshape(rounds, group, TOK_DEV)
    clusters = cluster_ids.reshape(HEADS, rounds, group, TOK_DEV).transpose(1, 2, 0, 3)

    def advance(totals, sliced):
        block_in, block_grad, block_seg, block_mask, block_clus = sliced

        def local_fn(values, *weights):
            return forward(values, *weights, block_seg, block_mask, block_clus)
        result, pullback = jax.vjp(local_fn, block_in, *params)
        gradients = pullback(block_grad)
        totals = tuple((total + piece for total, piece in zip(totals, gradients[1:])))
        return (totals, (result, gradients[0]))
    zero_grads = tuple((jnp.zeros_like(weight) for weight in params))
    totals, (results, input_grads) = lax.scan(advance, zero_grads, (inputs, cotangents, segments, masks, clusters))
    layer_output = results.reshape(TOKENS, D).astype(jnp.bfloat16)
    input_grad = input_grads.reshape(TOKENS, D).astype(jnp.bfloat16)
    return (layer_output, input_grad, totals[2], totals[3], totals[6], totals[7], totals[0], totals[1], totals[4], totals[5])
```

```python
import jax
import jax.numpy as jnp
from jax import lax
from jax.sharding import PartitionSpec as P

HDIM = 64
CLUST = 100


epsilon = 1e-05
far_below = -1e30
highest = lax.Precision.HIGHEST


def norm_parts(values):
    row_mean = jnp.mean(values, axis=-1, keepdims=True)
    centred = values - row_mean
    variance = jnp.mean(centred * centred, axis=-1, keepdims=True)
    row_scale = lax.rsqrt(variance + epsilon)
    return (centred * row_scale, row_scale)


def norm_back(upstream, normal, row_scale):
    first_term = jnp.mean(upstream, axis=-1, keepdims=True)
    second_term = jnp.mean(upstream * normal, axis=-1, keepdims=True)
    return row_scale * (upstream - first_term - normal * second_term)


def attention_parts(query, keys, segment_ids, pad_mask, cluster_ids):
    live_rows = (pad_mask > 0).astype(jnp.float32)
    labels = jnp.arange(CLUST, dtype=jnp.int32)
    member = (cluster_ids[:, None, :] == labels[None, :, None]).astype(jnp.float32) * live_rows[
        None, None, :
    ]
    counts = jnp.sum(member, axis=-1)
    member_low = member.astype(jnp.bfloat16)
    centre = (
        jnp.einsum("hcs,she->hce", member_low, query, preferred_element_type=jnp.float32)
        / counts[:, :, None]
    ).astype(jnp.bfloat16)
    seg_float = segment_ids.astype(jnp.float32)
    doc_owner = jnp.einsum("hcs,s->hc", member, seg_float, precision=highest) / counts
    allowed = (jnp.abs(doc_owner[:, :, None] - seg_float[None, None, :]) < 0.5) & (
        pad_mask[None, None, :] > 0
    )
    scores = jnp.einsum(
        "hce,she->hcs", centre, keys, preferred_element_type=jnp.float32
    ) * HDIM ** (-0.5)
    masked = jnp.where(allowed, scores, far_below)
    return (member, member_low, counts, centre, masked)


def swap_head(piece):
    return lax.ppermute(piece, "head", [(0, 1), (1, 0)])


def gather_head(piece):
    other = swap_head(piece)
    first = lax.axis_index("head") == 0
    return jnp.concatenate(
        [jnp.where(first, piece, other), jnp.where(first, other, piece)], axis=1
    )


def scatter_head(part, local_width):
    mine = lax.axis_index("head")
    away = lax.dynamic_slice_in_dim(part, (1 - mine) * local_width, local_width, 1)
    kept = lax.dynamic_slice_in_dim(part, mine * local_width, local_width, 1)
    return kept + swap_head(away.astype(jnp.bfloat16)).astype(jnp.float32)


def sum_head(part):
    low = part.astype(jnp.bfloat16)
    return low.astype(jnp.float32) + swap_head(low).astype(jnp.float32)


def butterfly(total):
    size = lax.axis_size("dp")
    place = lax.axis_index("dp")
    bits = []
    step = 1
    while step < size:
        pairs = [(i, i ^ step) for i in range(size)]
        bit = (place // step) % 2
        half = total.shape[0] // 2
        if total.shape[0] % 2 == 0 and half >= 8:
            away = lax.dynamic_slice_in_dim(total, (1 - bit) * half, half, 0)
            kept = lax.dynamic_slice_in_dim(total, bit * half, half, 0)
            bits.append((bit, pairs))
            total = kept + lax.ppermute(away.astype(jnp.bfloat16), "dp", pairs).astype(
                jnp.float32
            )
        else:
            low = total.astype(jnp.bfloat16)
            total = low.astype(jnp.float32) + lax.ppermute(low, "dp", pairs).astype(jnp.float32)
        step *= 2
    low = total.astype(jnp.bfloat16)
    for bit, pairs in reversed(bits):
        other = lax.ppermute(low, "dp", pairs)
        low = jnp.concatenate(
            [jnp.where(bit == 0, low, other), jnp.where(bit == 0, other, low)], axis=0
        )
    return low.astype(jnp.float32)


def all_sum(total):
    size = lax.axis_size("dp")
    step = 1
    while step < size:
        total = total + lax.ppermute(total, "dp", [(i, i ^ step) for i in range(size)])
        step *= 2
    return total


def shards(
    layer_input,
    first_gain,
    first_shift,
    qkv_weight,
    out_weight,
    second_gain,
    second_shift,
    up_weight,
    down_weight,
    segment_ids,
    pad_mask,
    cluster_ids,
    output_grad,
):
    tokens, local_width = layer_input.shape
    head_count = cluster_ids.shape[0]
    score_scale = HDIM ** (-0.5)
    start = lax.axis_index("head") * local_width
    whole_in = gather_head(layer_input).astype(jnp.float32)
    first_hat, first_scale = norm_parts(whole_in)
    normed = (first_hat * first_gain + first_shift).astype(jnp.bfloat16)
    projected = jnp.einsum(
        "td,ide->ite", normed, qkv_weight, preferred_element_type=jnp.float32
    ).astype(jnp.bfloat16)
    head_parts = projected.reshape(3, tokens, head_count, HDIM)
    query, keys, values = (head_parts[0], head_parts[1], head_parts[2])
    member, member_low, counts, centre, masked = attention_parts(
        query, keys, segment_ids, pad_mask, cluster_ids
    )
    row_top = jnp.max(masked, axis=-1, keepdims=True)
    log_total = row_top + jnp.log(jnp.sum(jnp.exp(masked - row_top), axis=-1, keepdims=True))
    weights = jnp.exp(masked - log_total).astype(jnp.bfloat16)
    centre_out = jnp.einsum(
        "hcs,she->hce", weights, values, preferred_element_type=jnp.float32
    ).astype(jnp.bfloat16)
    mixture = (
        jnp.einsum("hcs,hce->she", member_low, centre_out, preferred_element_type=jnp.float32)
        .astype(jnp.bfloat16)
        .reshape(tokens, local_width)
    )
    branch_part = jnp.dot(mixture, out_weight, preferred_element_type=jnp.float32)
    branch = scatter_head(branch_part, local_width)
    residual = layer_input.astype(jnp.float32) + branch
    whole_res = gather_head(residual.astype(jnp.bfloat16)).astype(residual.dtype)
    second_hat, second_scale = norm_parts(whole_res)
    second = (second_hat * second_gain + second_shift).astype(jnp.bfloat16)
    hidden = jnp.dot(second, up_weight, preferred_element_type=jnp.float32)
    activated, gelu_back = jax.vjp(jax.nn.gelu, hidden)
    activated = activated.astype(jnp.bfloat16)
    ffn_part = jnp.dot(activated, down_weight, preferred_element_type=jnp.float32)
    ffn_out = scatter_head(ffn_part, local_width)
    layer_output = (residual + ffn_out).astype(jnp.bfloat16)
    whole_grad = gather_head(output_grad)
    down_grad = jnp.einsum("tf,td->fd", activated, whole_grad, preferred_element_type=jnp.float32)
    act_grad = jnp.einsum("td,fd->tf", whole_grad, down_weight, preferred_element_type=jnp.float32)
    hidden_grad = gelu_back(act_grad)[0].astype(jnp.bfloat16)
    up_grad = jnp.einsum("td,tf->df", second, hidden_grad, preferred_element_type=jnp.float32)
    second_part = jnp.einsum(
        "tf,df->td", hidden_grad, up_weight, preferred_element_type=jnp.float32
    )
    second_back = sum_head(second_part)
    second_gain_grad = jnp.sum(second_back * second_hat, axis=0)
    second_shift_grad = jnp.sum(second_back, axis=0)
    residual_grad = whole_grad.astype(jnp.float32) + norm_back(
        second_back * second_gain, second_hat, second_scale
    )
    branch_grad = residual_grad.astype(jnp.bfloat16)
    mix_weight_grad = jnp.einsum(
        "te,td->ed", mixture, branch_grad, preferred_element_type=jnp.float32
    )
    mixture_grad = jnp.einsum(
        "td,ed->te", branch_grad, out_weight, preferred_element_type=jnp.float32
    ).reshape(tokens, head_count, HDIM)
    centre_out_grad = jnp.einsum("hcs,she->hce", member, mixture_grad, precision=highest).astype(
        jnp.bfloat16
    )
    probs = jnp.exp(masked - log_total)
    prob_grad = jnp.einsum(
        "hce,she->hcs", centre_out_grad, values, preferred_element_type=jnp.float32
    )
    value_grad = jnp.einsum(
        "hcs,hce->she", weights, centre_out_grad, preferred_element_type=jnp.float32
    )
    score_grad = (probs * (prob_grad - jnp.sum(prob_grad * probs, axis=-1, keepdims=True))).astype(
        jnp.bfloat16
    )
    centre_grad = (
        jnp.einsum("hcs,she->hce", score_grad, keys, preferred_element_type=jnp.float32)
        * score_scale
    )
    key_grad = (
        jnp.einsum("hcs,hce->she", score_grad, centre, preferred_element_type=jnp.float32)
        * score_scale
    )
    query_grad = jnp.einsum(
        "hcs,hce->she", member, centre_grad / counts[:, :, None], precision=highest
    )
    proj_grad = (
        jnp.stack([query_grad, key_grad, value_grad])
        .reshape(3, tokens, local_width)
        .astype(jnp.bfloat16)
    )
    qkv_grad = jnp.einsum("td,ite->ide", normed, proj_grad, preferred_element_type=jnp.float32)
    first_part = jnp.einsum(
        "ite,ide->td", proj_grad, qkv_weight, preferred_element_type=jnp.float32
    )
    first_back = sum_head(first_part)
    first_gain_grad = jnp.sum(first_back * first_hat, axis=0)
    first_shift_grad = jnp.sum(first_back, axis=0)
    input_full = residual_grad + norm_back(first_back * first_gain, first_hat, first_scale)
    input_grad = lax.dynamic_slice_in_dim(input_full, start, local_width, 1).astype(jnp.bfloat16)
    qkv_total = butterfly(qkv_grad.reshape(-1, local_width)).reshape(qkv_grad.shape)
    mix_total = butterfly(mix_weight_grad)
    up_total = butterfly(up_grad)
    down_total = butterfly(down_grad)
    small = all_sum(
        jnp.stack([first_gain_grad, first_shift_grad, second_gain_grad, second_shift_grad])
    )
    first_gain_total, first_shift_total, second_gain_total, second_shift_total = small
    return (
        layer_output,
        input_grad,
        qkv_total,
        mix_total,
        up_total,
        down_total,
        first_gain_total,
        first_shift_total,
        second_gain_total,
        second_shift_total,
    )


def solution(mesh):
    placed = (
        P("dp", "head"),
        P(),
        P(),
        P(None, None, "head"),
        P("head", None),
        P(),
        P(),
        P(None, "head"),
        P("head", None),
        P("dp"),
        P("dp"),
        P("head", "dp"),
        P("dp", "head"),
    )
    return jax.shard_map(
        shards,
        mesh=mesh,
        in_specs=placed,
        out_specs=(
            P("dp", "head"),
            P("dp", "head"),
            P(None, None, "head"),
            P("head", None),
            P(None, "head"),
            P("head", None),
            P(),
            P(),
            P(),
            P(),
        ),
        check_vma=False,
    )
```

```python
import functools

import jax
import jax.numpy as jnp
from jax import lax
from jax.experimental import pallas as pl
from jax.experimental.pallas import tpu as pltpu
from jax.sharding import PartitionSpec as P

HDIM = 64
CLUST = 100
CPAD = 128
TILE = 256
CHUNK = 512
EPS = 1e-05
FAR = -1e30
SCALE = HDIM**-0.5
C0 = 0.7978845608028654
C1 = 0.044715 * C0
MESH = pl.DeviceIdType.MESH
f32, bf16, i32 = jnp.float32, jnp.bfloat16, jnp.int32


def nn(a, b):
    return lax.dot_general(a, b, (((1,), (0,)), ((), ())), preferred_element_type=f32)


def nt(a, b):
    return lax.dot_general(a, b, (((1,), (1,)), ((), ())), preferred_element_type=f32)


def tn(a, b):
    return lax.dot_general(a, b, (((0,), (0,)), ((), ())), preferred_element_type=f32)


def ds(start, size, unit=None):
    if isinstance(start, int):
        return pl.ds(start, size)
    return pl.ds(pl.multiple_of(start, size if unit is None else unit), size)


def loop(count, body):
    def step(i, carry):
        body(i)
        return carry

    lax.fori_loop(0, count, step, 0)


def plan(rows, order):
    steps = []
    for step in order:
        halve = (rows // 2) % 16 == 0
        if halve:
            rows //= 2
        steps.append((step, rows, halve))
    return steps


class Total:
    def __init__(self, rt, rows, cols, order, acc, base, sends, recvs, out):
        self.rt, self.cols, self.acc, self.base, self.out = rt, cols, acc, base, out
        self.steps = plan(rows, order)
        self.sends, self.recvs = sends, recvs
        self.copies = []
        self.back = []
        self.at = 0
        self.size = rows
        self.pos = 0

    def bit(self, k):
        return (self.rt.place // self.steps[k][0]) % 2

    def peer(self, k):
        return self.rt.across(self.steps[k][0])

    def send(self, k):
        rows = self.steps[k][1]
        copy = self.rt.remote(self.sends[k], self.recvs[k], self.peer(k))
        copy.start()
        self.copies.append(copy)

    def first_sent(self):
        self.send(0)
        self.size //= 2
        self.at = self.bit(0) * self.size

    def move(self):
        k = self.pos
        self.pos += 1
        n = len(self.steps)
        if k < n:
            self.copies[k].wait()
            rows, halve = self.steps[k][1], self.steps[k][2]
            recv = self.recvs[k]
            acc, base = self.acc, self.base
            unit = 16
            own = None if halve else self.sends[k]
            if k + 1 < n:
                nrows, nhalve = self.steps[k + 1][1], self.steps[k + 1][2]
                out = self.sends[k + 1]
                if nhalve:
                    bit = self.bit(k + 1)
                    away, kept = (1 - bit) * nrows, bit * nrows

                    def cast(i):
                        r = ds(away + i * unit, unit)
                        a = ds(base + away + i * unit, unit)
                        out[ds(i * unit, unit), :] = self.join(acc, a, recv, own, r).astype(bf16)

                    loop(nrows // unit, cast)
                    self.send(k + 1)

                    def add(i):
                        r = ds(kept + i * unit, unit)
                        a = ds(base + kept + i * unit, unit)
                        acc[a, :] = self.join(acc, a, recv, own, r)

                    loop(nrows // unit, add)
                    self.base = base + kept
                    self.at = self.at + kept
                    self.size = nrows
                else:

                    def both(i):
                        r = ds(i * unit, unit)
                        a = ds(base + i * unit, unit)
                        v = self.join(acc, a, recv, own, r)
                        acc[a, :] = v
                        out[r, :] = v.astype(bf16)

                    loop(nrows // unit, both)
                    self.send(k + 1)
            else:

                def last(i):
                    r = ds(i * unit, unit)
                    a = ds(base + i * unit, unit)
                    o = ds(self.at + i * unit, unit)
                    self.out[o, :] = self.join(acc, a, recv, own, r).astype(bf16)

                loop(rows // unit, last)
                self.todo = [j for j in range(n) if self.steps[j][2]]
                self.gather()
            return
        self.back[-1].wait()
        self.gather()

    def join(self, acc, a, recv, own, r):
        mine = acc[a, :] if own is None else own[r, :].astype(f32)
        return mine + recv[r, :].astype(f32)

    def gather(self):
        if self.back:
            j = self.todo.pop()
            self.at = self.at - self.bit(j) * self.steps[j][1]
            self.size *= 2
        if not self.todo:
            return
        j = self.todo[-1]
        rows = self.out.at[ds(self.at, self.size, 16), :]
        copy = self.rt.remote(rows, rows, self.peer(j))
        copy.start()
        self.back.append(copy)

    @property
    def left(self):
        return len(self.steps) + sum(s[2] for s in self.steps) - self.pos


class Runtime:
    def __init__(self, nbits, send_sem, recv_sem, local_sem):
        self.place = lax.axis_index("dp")
        self.hd = lax.axis_index("head")
        self.nbits = nbits
        self.send_sem, self.recv_sem, self.local_sem = send_sem, recv_sem, local_sem
        self.used = self.used_local = 0

    def across(self, step):
        bit = (self.place // step) % 2
        return (self.place + step * (1 - 2 * bit), self.hd)

    @property
    def beside(self):
        return (self.place, 1 - self.hd)

    def take(self, count=1):
        self.used += count
        return self.used - count

    def remote(self, src, dst, peer, sem=None):
        k = self.take() if sem is None else sem
        return pltpu.make_async_remote_copy(
            src_ref=src,
            dst_ref=dst,
            send_sem=self.send_sem.at[k],
            recv_sem=self.recv_sem.at[k],
            device_id=peer,
            device_id_type=MESH,
        )

    def local(self, src, dst, sem=None):
        if sem is None:
            sem = self.used_local
            self.used_local += 1
        return pltpu.make_async_copy(src, dst, self.local_sem.at[sem])

    def enter(self):
        barrier = pltpu.get_barrier_semaphore()
        peers = [self.beside] + [self.across(1 << k) for k in range(self.nbits)]
        for peer in peers:
            pl.semaphore_signal(barrier, inc=1, device_id=peer, device_id_type=MESH)
        pl.semaphore_wait(barrier, len(peers))


def layer_kernel(names, nbits, orders, *refs):
    (x_in, og_in, w_in, ow_in, up_in, dn_in, ids_in, gv_in) = refs[:8]
    (lo_out, ig_out, q_out, m_out, u_out, d_out, g_out) = refs[8:15]
    s = dict(zip(names, refs[15:]))
    T, DL = x_in.shape
    D, FL = up_in.shape
    HL = DL // HDIM
    NP = HL // 2
    tiles = T // TILE
    rt = Runtime(nbits, s["send_sem"], s["recv_sem"], s["local_sem"])
    hd = rt.hd
    core = rt.place % 2
    X, OG, NRM, QKV, W, OW, UP, DN = (s[n] for n in ("X", "OG", "NRM", "QKV", "W", "OW", "UP", "DN"))
    IDS, IDE, IDT, GV, STATS, AUX = (s[n] for n in ("IDS", "IDE", "IDT", "GV", "STATS", "AUX"))
    MIX, RES, SEC, ACT, HG = (s[n] for n in ("MIX", "RES", "SEC", "ACT", "HG"))
    MB, SB, DB, WB, CEN, CO = (s[n] for n in ("MB", "SB", "DB", "WB", "CEN", "CO"))
    SCOL = s["SCOL"]
    HB, AB, PB = SB.at[:, pl.ds(0, CHUNK)], DB.at[:, pl.ds(0, CHUNK)], DB.at[:, pl.ds(0, D)]
    mine = ds(hd * DL, DL, 128)
    away = ds((1 - hd) * DL, DL, 128)

    def x_local(m):
        rows = ds(m * TILE, TILE)
        return rt.local(x_in.at[rows, :], X.at[rows, mine], sem=m)

    def og_local():
        return rt.local(og_in, OG.at[:, mine], sem=tiles)

    for m in range(tiles):
        x_local(m).start()
    rt.used_local = tiles + 1
    cp_ids = rt.local(ids_in, IDS.at[hd])
    cp_ids.start()
    cp_gv = rt.local(gv_in, GV)
    cp_gv.start()
    cp_w = rt.local(w_in, W)
    cp_w.start()
    cp_ow = rt.local(ow_in, OW.at[ds(hd * DL, DL, 16), :])
    cp_ow.start()
    og_local().start()
    cp_up = rt.local(up_in, UP)
    cp_up.start()
    cp_dn = rt.local(dn_in, DN)
    cp_dn.start()

    rt.enter()

    k_x, k_og = rt.take(tiles), rt.take(tiles)

    def x_remote(m):
        rows = ds(m * TILE, TILE)
        return rt.remote(x_in.at[rows, :], X.at[rows, mine], rt.beside, sem=k_x + m)

    def og_remote(m):
        rows = ds(m * TILE, TILE)
        return rt.remote(og_in.at[rows, :], OG.at[rows, mine], rt.beside, sem=k_og + m)

    cp_idr = rt.remote(ids_in, IDS.at[hd], rt.beside)
    cp_idr.start()
    for m in range(tiles):
        x_remote(m).start()
    half = DL // 2
    cp_owr = rt.remote(
        ow_in.at[ds(core * half, half, 16), :],
        OW.at[ds(hd * DL + core * half, half, 16), :],
        rt.beside,
    )
    cp_owr.start()
    og_remote(0).start()
    og_remote(1).start()

    cp_ids.wait()
    cp_idr.wait()
    cp_gv.wait()
    for h in range(2):
        ids = IDS[h]
        keep = ids[7:8, :] > 0
        ide = jnp.where(keep, ids, -1)
        IDE[h] = ide
        IDT[:, h * 8 : h * 8 + 8] = jnp.transpose(ide)
    g1, b1, g2, b2 = (GV[i : i + 1, :] for i in range(4))

    def p1(m):
        x_local(m).wait()
        x_remote(m).wait()
        unit = 32

        def norm(i):
            r = ds(m * TILE + i * unit, unit)
            v = X[r, :].astype(f32)
            mean = jnp.mean(v, axis=1, keepdims=True)
            c = v - mean
            rs = lax.rsqrt(jnp.mean(c * c, axis=1, keepdims=True) + EPS)
            NRM[r, :] = (c * rs * GV[0:1, :] + GV[1:2, :]).astype(bf16)
            STATS[r, 0:1] = mean
            STATS[r, 1:2] = rs

        loop(TILE // unit, norm)
        rows = ds(m * TILE, TILE)
        for i in range(3):
            QKV[i, rows, :] = nn(NRM[rows, :], W[i]).astype(bf16)

    cp_w.wait()
    loop(tiles, p1)

    cp_owr.wait()
    relay = OW.at[ds((1 - hd) * DL + core * half, half, 16), :]
    cp_owc = rt.remote(relay, relay, rt.across(1))
    cp_owc.start()

    low = lax.broadcasted_iota(i32, (CPAD, 128), 1) < HDIM

    def split(v):
        zero = jnp.zeros_like(v)
        return jnp.concatenate([jnp.where(low, v, zero), jnp.where(low, zero, v)], axis=0)

    def fold(v):
        return jnp.where(low, v[:CPAD], v[CPAD:])

    def members(h, p):
        unit = 16
        for a in range(2):
            k = 2 * p + a

            def fill(i):
                row = IDE[h, k : k + 1, :]
                c = lax.broadcasted_iota(i32, (unit, T), 0) + i * unit
                MB[ds(a * CPAD + i * unit, unit), :] = jnp.where(row == c, 1.0, 0.0).astype(bf16)

            loop(CPAD // unit, fill)

    def columns(cols, p):
        lane = lax.broadcasted_iota(i32, (TILE, CPAD), 1)
        parts = []
        for a in range(2):
            k = 2 * p + a
            parts.append(jnp.where(cols[:, k : k + 1] == lane, 1.0, 0.0).astype(bf16))
        return jnp.concatenate(parts, axis=1)

    def own_ids(rows):
        return jnp.where(hd == 0, IDT[rows, 0:8], IDT[rows, 8:16])

    def masked_scores(p, r):
        seg = IDE[hd, 6:7, :].astype(f32)
        allowed = jnp.abs(AUX[p, r, 1:2] - seg) < 0.5
        return jnp.where(allowed, SB[r, :] * SCALE, FAR)

    co_sent = []
    for p in range(NP):
        lanes = pl.ds(p * 128, 128)
        members(hd, p)
        unit = 16

        def count(i):
            r = ds(i * unit, unit)
            v = MB[r, :].astype(f32)
            n = jnp.maximum(jnp.sum(v, axis=1, keepdims=True), 1.0)
            seg = IDE[hd, 6:7, :].astype(f32)
            AUX[p, r, 0:1] = 1.0 / n
            AUX[p, r, 1:2] = jnp.sum(v * seg, axis=1, keepdims=True) / n

        loop(2 * CPAD // unit, count)
        cen = (nn(MB[...], QKV[0, :, lanes]) * AUX[p, :, 0:1]).astype(bf16)
        CEN[p] = split(fold(cen))
        SB[...] = nt(CEN[p], QKV[1, :, lanes])

        def soft(i):
            r = ds(i * unit, unit)
            v = masked_scores(p, r)
            top = jnp.max(v, axis=1, keepdims=True)
            e = jnp.exp(v - top)
            den = jnp.sum(e, axis=1, keepdims=True)
            WB[r, :] = (e * (1.0 / den)).astype(bf16)
            AUX[p, r, 2:3] = top + jnp.log(den)

        loop(2 * CPAD // unit, soft)
        CO[hd * NP + p] = fold(nn(WB[...], QKV[2, :, lanes]).astype(bf16))
        there = CO.at[hd * NP + p]
        copy = rt.remote(there, there, rt.beside)
        copy.start()
        co_sent.append(copy)

    for m in range(2, tiles):
        og_remote(m).start()

    cp_ow.wait()
    cp_owc.wait()
    for copy in co_sent:
        copy.wait()

    def p3(m):
        rows = ds(m * TILE, TILE)
        for q in range(2 * NP):
            h, p = q // NP, q % NP
            MIX[rows, q * 128 : (q + 1) * 128] = nn(columns(IDT[rows, h * 8 : h * 8 + 8], p), split(CO[q])).astype(bf16)
        PB[...] = nn(MIX[rows, :], OW[...])
        unit = 32

        def norm(i):
            r = ds(m * TILE + i * unit, unit)
            v = X[r, :].astype(f32) + PB[ds(i * unit, unit), :]
            RES[r, :] = v
            mean = jnp.mean(v, axis=1, keepdims=True)
            c = v - mean
            rs = lax.rsqrt(jnp.mean(c * c, axis=1, keepdims=True) + EPS)
            SEC[r, :] = (c * rs * GV[2:3, :] + GV[3:4, :]).astype(bf16)
            STATS[r, 2:3] = mean
            STATS[r, 3:4] = rs

        loop(TILE // unit, norm)

    loop(tiles, p3)

    cp_up.wait()
    cp_dn.wait()
    og_local().wait()
    S2, S2S, S2R, STS, STR = (s[n] for n in ("S2", "S2S", "S2R", "STS", "STR"))
    k_s2, k_st = rt.take(tiles), rt.take(tiles)

    def s2_remote(m):
        rows = ds(m * TILE, TILE)
        return rt.remote(S2S.at[rows, :], S2R.at[rows, :], rt.beside, sem=k_s2 + m)

    def st_remote(m):
        return rt.remote(STS.at[m], STR.at[m], rt.beside, sem=k_st + m)

    def row_sums(m, own, send, out, gain, src, k):
        unit = 32

        def split_rows(i):
            r = ds(m * TILE + i * unit, unit)
            b = ds(i * unit, unit)
            own[r, :] = PB[b, mine]
            send[r, :] = PB[b, away].astype(bf16)
            e = PB[b, :] * GV[gain : gain + 1, :]
            nh = (src[r, :].astype(f32) - STATS[r, k : k + 1]) * STATS[r, k + 1 : k + 2]
            SCOL[b, 0:1] = jnp.sum(e, axis=1, keepdims=True)
            SCOL[b, 1:2] = jnp.sum(e * nh, axis=1, keepdims=True)

        loop(TILE // unit, split_rows)
        out[m] = jnp.transpose(SCOL[...])[0:8, :]

    SCOL[...] = jnp.zeros_like(SCOL)

    def p4(m):
        og_remote(m).wait()
        rows = ds(m * TILE, TILE)

        def chunk(n):
            cols = ds(n * CHUNK, CHUNK)
            HB[...] = nn(SEC[rows, :], UP[:, cols])
            AB[...] = nt(OG[rows, :], DN[cols, :])
            unit = 16

            def gelu(i):
                b = ds(i * unit, unit)
                r = ds(m * TILE + i * unit, unit)
                v = HB[b, :]
                v2 = v * v
                t = jnp.tanh(v * (C0 + C1 * v2))
                hf = 0.5 * t + 0.5
                act = v * hf
                slope = hf + act * (1.0 - hf) * (2 * C0 + 6 * C1 * v2)
                ACT[r, cols] = act.astype(bf16)
                HG[r, cols] = (AB[b, :] * slope).astype(bf16)

            loop(TILE // unit, gelu)

        loop(FL // CHUNK, chunk)
        PB[...] = nt(HG[rows, :], UP[...])
        row_sums(m, S2, S2S, STS, 2, RES, 2)
        s2_remote(m).start()
        st_remote(m).start()

    loop(tiles, p4)

    def total(name, rows, cols, order, acc, base=0, sends=None):
        steps = plan(rows, order)
        count = len(steps)
        if sends is None:
            sends = [s[f"{name}S{k}"] for k in range(count)]
        recvs = [s[f"{name}R{k}"] for k in range(count)]
        return Total(rt, rows, cols, order, acc, base, sends, recvs, s[f"{name}O"])

    dg = total("D", FL, D, orders[0], s["DA"])
    ug_sends = [dg.sends[0]] + [s[f"US{k}"] for k in range(1, len(plan(FL, orders[1])))]
    ug = total("U", FL, D, orders[1], s["UA"], sends=ug_sends)

    def grad_half(left, right, first, rows, tall, store):
        def one(j):
            cols = ds(first + j * tall, tall, 128)
            store(ds(j * tall, tall), tn(left[:, cols], right))

        loop(rows // tall, one)

    def to_low(ref):
        def store(r, v):
            ref[r, :] = v.astype(bf16)

        return store

    def to_full(ref):
        def store(r, v):
            ref[r, :] = v

        return store

    grad_half(ACT, OG[...], (1 - core) * (FL // 2), FL // 2, 384, to_low(dg.sends[0]))
    dg.first_sent()
    grad_half(ACT, OG[...], core * (FL // 2), FL // 2, 384, to_full(dg.acc))
    dg.move()
    hg_half = lambda c: HG[:, ds(c * (FL // 2), FL // 2, 128)]
    grad_half(SEC, hg_half(1 - core), 0, D, 384, to_low(ug.sends[0]))
    ug.first_sent()
    grad_half(SEC, hg_half(core), 0, D, 384, to_full(ug.acc))
    ug.move()

    BG, GACC, MG = HG.at[:, pl.ds(3 * DL, DL)], s["GACC"], SEC
    GACC[...] = jnp.zeros_like(GACC)

    def norm_back(m, own, recv, sums, got, gain, src, k, base, write, slot):
        unit = 16
        SCOL[...] = jnp.transpose(
            jnp.concatenate([sums[m] + got[m], jnp.zeros((120, TILE), f32)], axis=0)
        ) * (1.0 / D)

        def rowsback(i):
            r = ds(m * TILE + i * unit, unit)
            b = ds(i * unit, unit)
            e = own[r, :] + recv[r, :].astype(f32)
            nh = (src[r, mine].astype(f32) - STATS[r, k : k + 1]) * STATS[r, k + 1 : k + 2]
            grad = STATS[r, k + 1 : k + 2] * (
                e * GV[gain : gain + 1, mine] - SCOL[b, 0:1] - nh * SCOL[b, 1:2]
            )
            write(r, base(r) + grad)
            en = e * nh
            GACC[slot] += en[0:8] + en[8:16]
            GACC[slot + 1] += e[0:8] + e[8:16]

        loop(TILE // unit, rowsback)

    def p5(m):
        s2_remote(m).wait()
        st_remote(m).wait()

        def write(r, v):
            S2[r, :] = v
            BG[r, :] = v.astype(bf16)

        norm_back(m, S2, S2R, STS, STR, 2, RES, 2, lambda r: OG[r, mine].astype(f32), write, 2)
        rows = ds(m * TILE, TILE)
        MG[rows, :] = nt(BG[rows, :], OW[:, mine]).astype(bf16)

    loop(tiles, p5)

    CGS, CGR, CGO = s["CGS"], s["CGR"], s["CGO"]

    def reduce_pair(h, p):
        members(h, p)
        lanes = ds((h * NP + p) * 128, 128)
        return fold(nn(MB[...], MG[:, lanes]))

    for p in range(NP):
        CGS[p] = reduce_pair(1 - hd, p)
    cp_cg = rt.remote(CGS, CGR, rt.beside)
    cp_cg.start()

    MA, MXS, MXR = s["MA"], MIX.at[pl.ds(0, DL), away], s["MXR"]
    MXS[...] = tn(MIX[:, away], BG[...]).astype(bf16)
    cp_mx = rt.remote(MXS, MXR, rt.beside)
    cp_mx.start()
    for p in range(NP):
        CGO[p] = reduce_pair(hd, p)
    MA[ds(hd * DL, DL, 16), :] = tn(MIX[:, mine], BG[...])

    dg.move()

    FFS, FFR = MIX.at[:, mine], s["FFR"]
    k_ff = rt.take(tiles)

    def ff_remote(m):
        rows = ds(m * TILE, TILE)
        return rt.remote(FFS.at[rows, :], FFR.at[rows, :], rt.beside, sem=k_ff + m)

    def p6(m):
        rows = ds(m * TILE, TILE)
        PB[...] = nn(ACT[rows, :], DN[...])
        unit = 32

        def split_rows(i):
            r = ds(m * TILE + i * unit, unit)
            b = ds(i * unit, unit)
            RES[r, mine] += PB[b, mine]
            FFS[r, :] = PB[b, away].astype(bf16)

        loop(TILE // unit, split_rows)
        ff_remote(m).start()

    loop(tiles, p6)
    ug.move()

    PG = HG
    cp_cg.wait()
    for p in range(NP):
        lanes = pl.ds(p * 128, 128)
        cog = split((CGO[p] + CGR[p]).astype(bf16))
        SB[...] = nt(CEN[p], QKV[1, :, lanes])
        DB[...] = nt(cog, QKV[2, :, lanes])
        unit = 16

        def back(i):
            r = ds(i * unit, unit)
            pr = jnp.exp(masked_scores(p, r) - AUX[p, r, 2:3])
            WB[r, :] = pr.astype(bf16)
            dp = DB[r, :]
            dot = jnp.sum(dp * pr, axis=1, keepdims=True)
            MB[r, :] = (pr * (dp - dot)).astype(bf16)

        loop(2 * CPAD // unit, back)
        cg = (nn(MB[...], QKV[1, :, lanes]) * (SCALE * AUX[p, :, 0:1])).astype(bf16)
        cg = split(fold(cg))
        for m in range(tiles):
            rows = pl.ds(m * TILE, TILE)
            at = p * 128
            PG[rows, at : at + 128] = nn(columns(own_ids(rows), p), cg).astype(bf16)
            PG[rows, DL + at : DL + at + 128] = (tn(MB[:, rows], CEN[p]) * SCALE).astype(bf16)
            PG[rows, 2 * DL + at : 2 * DL + at + 128] = tn(WB[:, rows], cog).astype(bf16)

    F1, F1S, F1R = RES.at[:, away], S2S, s["F1R"]
    FTS, FTR = s["FTS"], s["FTR"]
    k_f1, k_ft = rt.take(tiles), rt.take(tiles)

    def f1_remote(m):
        rows = ds(m * TILE, TILE)
        return rt.remote(F1S.at[rows, :], F1R.at[rows, :], rt.beside, sem=k_f1 + m)

    def ft_remote(m):
        return rt.remote(FTS.at[m], FTR.at[m], rt.beside, sem=k_ft + m)

    def p8(m):
        rows = ds(m * TILE, TILE)
        acc = nt(PG[rows, 0:DL], W[0])
        acc += nt(PG[rows, DL : 2 * DL], W[1])
        acc += nt(PG[rows, 2 * DL : 3 * DL], W[2])
        PB[...] = acc
        row_sums(m, F1, F1S, FTS, 0, X, 0)
        f1_remote(m).start()
        ft_remote(m).start()

    loop(tiles, p8)
    dg.move()

    def act_sends(rows, order, block):
        sends, at = [], 0
        for step, count, halve in plan(rows, order):
            sends.append(ACT.at[pl.ds(at, count), pl.ds(block * DL, DL)])
            at += count
        return sends

    grads = []
    for i in (2, 1, 0):
        name = "QKV"[i]
        tot = total(name, D, DL, orders[2 + i], s[f"{name}A"], 0, act_sends(D, orders[2 + i], i))
        right = PG[:, i * DL : (i + 1) * DL]
        grad_half(NRM, right, (1 - core) * (D // 2), D // 2, 384, to_low(tot.sends[0]))
        tot.first_sent()
        grad_half(NRM, right, core * (D // 2), D // 2, 384, to_full(tot.acc))
        grads.append(tot)
    vg, kg, qg = grads
    cp_mx.wait()
    mg = total("M", D, DL, orders[5], MA, core * DL, act_sends(D, orders[5], 3))

    def spread(i):
        MA[ds((1 - hd) * DL + i * 16, 16), :] = MXR[ds(i * 16, 16), :].astype(f32)

    loop(DL // 16, spread)

    def mix_half(i):
        mg.sends[0][ds(i * 16, 16), :] = MA[ds((1 - core) * DL + i * 16, 16), :].astype(bf16)

    loop(DL // 16, mix_half)
    mg.first_sent()
    for tot in (vg, kg, qg, mg):
        tot.move()
    ug.move()
    dg.move()

    LO, IG = S2R, BG

    def p9(m):
        ff_remote(m).wait()
        unit = 32

        def rows_out(i):
            r = ds(m * TILE + i * unit, unit)
            LO[r, :] = (RES[r, mine] + FFR[r, :].astype(f32)).astype(bf16)

        loop(TILE // unit, rows_out)

    loop(tiles, p9)
    cp_lo = rt.local(LO, lo_out)
    cp_lo.start()
    for tot in (ug, dg, vg, kg, qg, mg):
        tot.move()

    def p10(m):
        f1_remote(m).wait()
        ft_remote(m).wait()

        def write(r, v):
            IG[r, :] = v.astype(bf16)

        norm_back(m, F1, F1R, FTS, FTR, 0, X, 0, lambda r: S2[r, :], write, 0)

    loop(tiles, p10)
    cp_ig = rt.local(IG, ig_out)
    cp_ig.start()

    GX, GR, GO = s["GX"], s["GR"], s["GO"]
    for k in range(4):
        GX[0, k : k + 1, :] = jnp.sum(GACC[k], axis=0, keepdims=True)
    GX[0, 4:8, :] = jnp.zeros((4, DL), f32)
    done = [cp_lo, cp_ig]

    def finish(tot, src, dst):
        copy = rt.local(src, dst)
        copy.start()
        done.append(copy)

    totals = [
        (dg, lambda: finish(dg, s["DO"], d_out)),
        (ug, lambda: [finish(ug, s["UO"].at[pl.ds(j * D, D), :], u_out.at[:, pl.ds(j * D, D)]) for j in range(2)]),
        (vg, lambda: finish(vg, s["VO"], q_out.at[2])),
        (kg, lambda: finish(kg, s["KO"], q_out.at[1])),
        (qg, lambda: finish(qg, s["QO"], q_out.at[0])),
        (mg, lambda: [finish(mg, s["MO"].at[pl.ds(j * DL, DL), :], m_out.at[:, pl.ds(j * DL, DL)]) for j in range(2)]),
    ]
    gain_copy = None
    gain_step = 0

    def gain_move():
        nonlocal gain_copy, gain_step
        if gain_step > nbits + 1:
            return
        if gain_copy is not None:
            gain_copy.wait()
            if gain_step <= nbits:
                GX[gain_step] = GX[gain_step - 1] + GR[gain_step - 1]
            else:
                GO[:, away] = GR[nbits]
                GO[:, mine] = GX[nbits]
                copy = rt.local(GO, g_out)
                copy.start()
                done.append(copy)
        if gain_step < nbits:
            gain_copy = rt.remote(GX.at[gain_step], GR.at[gain_step], rt.across(1 << gain_step))
            gain_copy.start()
        elif gain_step == nbits:
            gain_copy = rt.remote(GX.at[nbits], GR.at[nbits], rt.beside)
            gain_copy.start()
        gain_step += 1

    gain_move()
    while any(tot.left for tot, _ in totals):
        for tot, end in totals:
            if tot.left:
                tot.move()
                if not tot.left:
                    end()
        gain_move()
    while gain_step <= nbits + 1:
        gain_move()
    for copy in done:
        copy.wait()


def layer(nbits, args):
    x, og, w, ow, up, dn, ids, gv = args
    T, DL = x.shape
    D, FL = up.shape
    NP = DL // 128
    bits = [1 << k for k in range(nbits)]
    order_a = list(bits)
    order_b = [bits[0]] + ([bits[2], bits[1]] + bits[3:] if nbits > 2 else bits[1:])
    orders = [order_a, order_b, order_a, order_b, order_a, order_b]
    tiles = T // TILE
    V = pltpu.VMEM
    scratch = [
        ("X", V((T, D), bf16)),
        ("OG", V((T, D), bf16)),
        ("NRM", V((T, D), bf16)),
        ("QKV", V((3, T, DL), bf16)),
        ("W", V((3, D, DL), bf16)),
        ("OW", V((D, D), bf16)),
        ("UP", V((D, FL), bf16)),
        ("DN", V((FL, D), bf16)),
        ("IDS", V((2, 8, T), i32)),
        ("IDE", V((2, 8, T), i32)),
        ("IDT", V((T, 16), i32)),
        ("GV", V((4, D), f32)),
        ("STATS", V((T, 8), f32)),
        ("AUX", V((NP, 2 * CPAD, 8), f32)),
        ("MIX", V((T, D), bf16)),
        ("RES", V((T, D), f32)),
        ("SEC", V((T, D), bf16)),
        ("ACT", V((T, FL), bf16)),
        ("HG", V((T, FL), bf16)),
        ("MB", V((2 * CPAD, T), bf16)),
        ("SB", V((2 * CPAD, T), f32)),
        ("DB", V((2 * CPAD, T), f32)),
        ("WB", V((2 * CPAD, T), bf16)),
        ("CEN", V((NP, 2 * CPAD, 128), bf16)),
        ("CO", V((2 * NP, CPAD, 128), bf16)),
        ("SCOL", V((TILE, 128), f32)),
        ("S2", V((T, DL), f32)),
        ("S2S", V((T, DL), bf16)),
        ("S2R", V((T, DL), bf16)),
        ("STS", V((tiles, 8, TILE), f32)),
        ("STR", V((tiles, 8, TILE), f32)),
        ("GACC", V((4, 8, DL), f32)),
        ("CGS", V((NP, CPAD, 128), f32)),
        ("CGR", V((NP, CPAD, 128), f32)),
        ("CGO", V((NP, CPAD, 128), f32)),
        ("MA", V((D, DL), f32)),
        ("MXR", V((DL, DL), bf16)),
        ("FFR", V((T, DL), bf16)),
        ("F1R", V((T, DL), bf16)),
        ("FTS", V((tiles, 8, TILE), f32)),
        ("FTR", V((tiles, 8, TILE), f32)),
        ("GX", V((nbits + 1, 8, DL), f32)),
        ("GR", V((nbits + 1, 8, DL), f32)),
        ("GO", V((8, D), f32)),
        ("DA", V((FL // 2, D), f32)),
        ("UA", V((D, FL // 2), f32)),
        ("QA", V((D // 2, DL), f32)),
        ("KA", V((D // 2, DL), f32)),
        ("VA", V((D // 2, DL), f32)),
    ]
    for name, rows, cols, order, own in (
        ("D", FL, D, orders[0], True),
        ("U", FL, D, orders[1], True),
        ("Q", D, DL, orders[2], False),
        ("K", D, DL, orders[3], False),
        ("V", D, DL, orders[4], False),
        ("M", D, DL, orders[5], False),
    ):
        for k, (step, count, halve) in enumerate(plan(rows, order)):
            if own and (name, k) != ("U", 0):
                scratch.append((f"{name}S{k}", V((count, cols), bf16)))
            scratch.append((f"{name}R{k}", V((count, cols), bf16)))
        scratch.append((f"{name}O", V((rows, cols), bf16)))
    copies = 6 * tiles + 16 + NP + 12 * nbits + nbits
    scratch += [
        ("send_sem", pltpu.SemaphoreType.DMA((copies,))),
        ("recv_sem", pltpu.SemaphoreType.DMA((copies,))),
        ("local_sem", pltpu.SemaphoreType.DMA((tiles + 24,))),
    ]
    shape = jax.ShapeDtypeStruct
    hbm = pl.BlockSpec(memory_space=pl.ANY)
    return pl.pallas_call(
        functools.partial(layer_kernel, [n for n, _ in scratch], nbits, orders),
        out_shape=(
            shape((T, DL), bf16),
            shape((T, DL), bf16),
            shape((3, D, DL), bf16),
            shape((DL, D), bf16),
            shape((D, FL), bf16),
            shape((FL, D), bf16),
            shape((8, D), f32),
        ),
        in_specs=[hbm] * 8,
        out_specs=(hbm,) * 7,
        scratch_shapes=[v for _, v in scratch],
        compiler_params=pltpu.CompilerParams(
            collective_id=0, has_side_effects=True, vmem_limit_bytes=67043328
        ),
        name="layer",
    )(x, og, w, ow, up, dn, ids, gv)


def shards(
    nbits,
    layer_input,
    first_gain,
    first_shift,
    qkv_weight,
    out_weight,
    second_gain,
    second_shift,
    up_weight,
    down_weight,
    segment_ids,
    pad_mask,
    cluster_ids,
    output_grad,
):
    ids = jnp.concatenate([cluster_ids, segment_ids[None], pad_mask[None]], axis=0)
    gains = jnp.stack([first_gain, first_shift, second_gain, second_shift])
    lo, ig, q, m, u, d, g = layer(
        nbits,
        (layer_input, output_grad, qkv_weight, out_weight, up_weight, down_weight, ids, gains),
    )
    return (lo, ig, q.astype(f32), m.astype(f32), u.astype(f32), d.astype(f32), g[0], g[1], g[2], g[3])


def solution(mesh):
    nbits = mesh.shape["dp"].bit_length() - 1
    placed = (
        P("dp", "head"),
        P(),
        P(),
        P(None, None, "head"),
        P("head", None),
        P(),
        P(),
        P(None, "head"),
        P("head", None),
        P("dp"),
        P("dp"),
        P("head", "dp"),
        P("dp", "head"),
    )
    return jax.shard_map(
        functools.partial(shards, nbits),
        mesh=mesh,
        in_specs=placed,
        out_specs=(
            P("dp", "head"),
            P("dp", "head"),
            P(None, None, "head"),
            P("head", None),
            P(None, "head"),
            P("head", None),
            P(),
            P(),
            P(),
            P(),
        ),
        check_vma=False,
    )
```

```python
import functools

import jax
import jax.numpy as jnp
from jax import lax
from jax.experimental import pallas as pl
from jax.experimental.pallas import tpu as pltpu
from jax.sharding import PartitionSpec as P

HDIM = 64
CLUST = 100
CPAD = 128
TILE = 256
CHUNK = 512
UN, UA, UG = 8, 16, 16
SCHED = {"r": "D", "f": "U", "b0": "D", "b1": "U", "b2": "D", "o": "U", "v": "D", "k": "VU", "q": "K", "m": "QDV", "l": "MUKQ", "e": "DVM"}
EPS = 1e-05
FAR = -1e30
SCALE = HDIM**-0.5
C0 = 0.7978845608028654
C1 = 0.044715 * C0
MESH = pl.DeviceIdType.MESH
f32, bf16, i32 = jnp.float32, jnp.bfloat16, jnp.int32


def nn(a, b):
    return lax.dot_general(a, b, (((1,), (0,)), ((), ())), preferred_element_type=f32)


def nt(a, b):
    return lax.dot_general(a, b, (((1,), (1,)), ((), ())), preferred_element_type=f32)


def tn(a, b):
    return lax.dot_general(a, b, (((0,), (0,)), ((), ())), preferred_element_type=f32)


def ds(start, size, unit=None):
    if isinstance(start, int):
        return pl.ds(start, size)
    return pl.ds(pl.multiple_of(start, size if unit is None else unit), size)


def loop(count, body, unroll=1):
    while count % unroll:
        unroll -= 1
    if count == unroll:
        for i in range(count):
            body(i)
        return

    def step(i, carry):
        for j in range(unroll):
            body(i * unroll + j)
        return carry

    lax.fori_loop(0, count // unroll, step, 0)


def plan(rows, order):
    steps = []
    for step in order:
        halve = (rows // 2) % 16 == 0
        if halve:
            rows //= 2
        steps.append((step, rows, halve))
    return steps


class Total:
    def __init__(self, rt, rows, cols, order, acc, base, sends, recvs, out):
        self.rt, self.cols, self.acc, self.base, self.out = rt, cols, acc, base, out
        self.steps = plan(rows, order)
        self.sends, self.recvs = sends, recvs
        self.copies = []
        self.back = []
        self.at = 0
        self.size = rows
        self.pos = 0

    def bit(self, k):
        return (self.rt.place // self.steps[k][0]) % 2

    def peer(self, k):
        return self.rt.across(self.steps[k][0])

    def send(self, k):
        rows = self.steps[k][1]
        copy = self.rt.remote(self.sends[k], self.recvs[k], self.peer(k))
        copy.start()
        self.copies.append(copy)

    def first_sent(self):
        self.send(0)
        self.size //= 2
        self.at = self.bit(0) * self.size

    def move(self):
        k = self.pos
        self.pos += 1
        n = len(self.steps)
        if k < n:
            self.copies[k].wait()
            rows, halve = self.steps[k][1], self.steps[k][2]
            recv = self.recvs[k]
            acc, base = self.acc, self.base
            unit = 16
            own = None if halve else self.sends[k]
            if k + 1 < n:
                nrows, nhalve = self.steps[k + 1][1], self.steps[k + 1][2]
                out = self.sends[k + 1]
                if nhalve:
                    bit = self.bit(k + 1)
                    away, kept = (1 - bit) * nrows, bit * nrows

                    def cast(i):
                        r = ds(away + i * unit, unit)
                        a = ds(base + away + i * unit, unit)
                        out[ds(i * unit, unit), :] = self.join(acc, a, recv, own, r).astype(bf16)

                    loop(nrows // unit, cast, 4)
                    self.send(k + 1)

                    def add(i):
                        r = ds(kept + i * unit, unit)
                        a = ds(base + kept + i * unit, unit)
                        acc[a, :] = self.join(acc, a, recv, own, r)

                    loop(nrows // unit, add, 4)
                    self.base = base + kept
                    self.at = self.at + kept
                    self.size = nrows
                else:

                    def both(i):
                        r = ds(i * unit, unit)
                        a = ds(base + i * unit, unit)
                        v = self.join(acc, a, recv, own, r)
                        acc[a, :] = v
                        out[r, :] = v.astype(bf16)

                    loop(nrows // unit, both, 4)
                    self.send(k + 1)
            else:

                def last(i):
                    r = ds(i * unit, unit)
                    a = ds(base + i * unit, unit)
                    o = ds(self.at + i * unit, unit)
                    self.out[o, :] = self.join(acc, a, recv, own, r).astype(bf16)

                loop(rows // unit, last, 4)
                self.todo = [j for j in range(n) if self.steps[j][2]]
                self.gather()
            return
        self.back[-1].wait()
        self.gather()

    def join(self, acc, a, recv, own, r):
        mine = acc[a, :] if own is None else own[r, :].astype(f32)
        return mine + recv[r, :].astype(f32)

    def gather(self):
        if self.back:
            j = self.todo.pop()
            self.at = self.at - self.bit(j) * self.steps[j][1]
            self.size *= 2
        if not self.todo:
            return
        j = self.todo[-1]
        rows = self.out.at[ds(self.at, self.size, 16), :]
        copy = self.rt.remote(rows, rows, self.peer(j))
        copy.start()
        self.back.append(copy)

    @property
    def left(self):
        return len(self.steps) + sum(s[2] for s in self.steps) - self.pos


class Runtime:
    def __init__(self, nbits, send_sem, recv_sem, local_sem):
        self.place = lax.axis_index("dp")
        self.hd = lax.axis_index("head")
        self.nbits = nbits
        self.send_sem, self.recv_sem, self.local_sem = send_sem, recv_sem, local_sem
        self.used = self.used_local = 0

    def across(self, step):
        bit = (self.place // step) % 2
        return (self.place + step * (1 - 2 * bit), self.hd)

    @property
    def beside(self):
        return (self.place, 1 - self.hd)

    def take(self, count=1):
        self.used += count
        return self.used - count

    def remote(self, src, dst, peer, sem=None):
        k = self.take() if sem is None else sem
        return pltpu.make_async_remote_copy(
            src_ref=src,
            dst_ref=dst,
            send_sem=self.send_sem.at[k],
            recv_sem=self.recv_sem.at[k],
            device_id=peer,
            device_id_type=MESH,
        )

    def local(self, src, dst, sem=None):
        if sem is None:
            sem = self.used_local
            self.used_local += 1
        return pltpu.make_async_copy(src, dst, self.local_sem.at[sem])

    def enter(self):
        barrier = pltpu.get_barrier_semaphore()
        peers = [self.beside] + [self.across(1 << k) for k in range(self.nbits)]
        for peer in peers:
            pl.semaphore_signal(barrier, inc=1, device_id=peer, device_id_type=MESH)
        pl.semaphore_wait(barrier, len(peers))


def layer_kernel(names, nbits, orders, *refs):
    (x_in, og_in, w_in, ow_in, up_in, dn_in, ids_in, gv_in) = refs[:8]
    (lo_out, ig_out, q_out, m_out, u_out, d_out, g_out) = refs[8:15]
    s = dict(zip(names, refs[15:]))
    T, DL = x_in.shape
    D, FL = up_in.shape
    HL = DL // HDIM
    NP = HL // 2
    tiles = T // TILE
    rt = Runtime(nbits, s["send_sem"], s["recv_sem"], s["local_sem"])
    hd = rt.hd
    core = rt.place % 2
    X, OG, NRM, QKV, W, OW, UP, DN = (s[n] for n in ("X", "OG", "NRM", "QKV", "W", "OW", "UP", "DN"))
    IDS, IDE, IDT, GV, STATS, AUX = (s[n] for n in ("IDS", "IDE", "IDT", "GV", "STATS", "AUX"))
    MIX, RES, SEC, ACT, HG = (s[n] for n in ("MIX", "RES", "SEC", "ACT", "HG"))
    MB, SB, DB, WB, CEN, CO = (s[n] for n in ("MB", "SB", "DB", "WB", "CEN", "CO"))
    SCOL = s["SCOL"]
    HB, AB, PB = SB.at[:, pl.ds(0, CHUNK)], DB.at[:, pl.ds(0, CHUNK)], DB.at[:, pl.ds(0, D)]
    mine = ds(hd * DL, DL, 128)
    away = ds((1 - hd) * DL, DL, 128)

    def x_local(m):
        rows = ds(m * TILE, TILE)
        return rt.local(x_in.at[rows, :], X.at[rows, mine], sem=m)

    def og_local():
        return rt.local(og_in, OG.at[:, mine], sem=tiles)

    for m in range(tiles):
        x_local(m).start()
    rt.used_local = tiles + 1
    cp_ids = rt.local(ids_in, IDS.at[hd])
    cp_ids.start()
    cp_gv = rt.local(gv_in, GV)
    cp_gv.start()
    cp_w = rt.local(w_in, W)
    cp_w.start()
    cp_ow = rt.local(ow_in, OW.at[ds(hd * DL, DL, 16), :])
    cp_ow.start()
    og_local().start()
    cp_up = rt.local(up_in, UP)
    cp_up.start()
    cp_dn = rt.local(dn_in, DN)
    cp_dn.start()

    rt.enter()

    k_x, k_og = rt.take(tiles), rt.take(tiles)

    def x_remote(m):
        rows = ds(m * TILE, TILE)
        return rt.remote(x_in.at[rows, :], X.at[rows, mine], rt.beside, sem=k_x + m)

    def og_remote(m):
        rows = ds(m * TILE, TILE)
        return rt.remote(og_in.at[rows, :], OG.at[rows, mine], rt.beside, sem=k_og + m)

    cp_idr = rt.remote(ids_in, IDS.at[hd], rt.beside)
    cp_idr.start()
    for m in range(tiles):
        x_remote(m).start()
    half = DL // 2
    cp_owr = rt.remote(
        ow_in.at[ds(core * half, half, 16), :],
        OW.at[ds(hd * DL + core * half, half, 16), :],
        rt.beside,
    )
    cp_owr.start()

    cp_ids.wait()
    cp_idr.wait()
    cp_gv.wait()
    for h in range(2):
        ids = IDS[h]
        keep = ids[7:8, :] > 0
        ide = jnp.where(keep, ids, -1)
        IDE[h] = ide
        IDT[:, h * 8 : h * 8 + 8] = jnp.transpose(ide)
    g1, b1, g2, b2 = (GV[i : i + 1, :] for i in range(4))

    def p1(m):
        x_local(m).wait()
        x_remote(m).wait()
        unit = 32

        def norm(i):
            r = ds(m * TILE + i * unit, unit)
            v = X[r, :].astype(f32)
            mean = jnp.mean(v, axis=1, keepdims=True)
            c = v - mean
            rs = lax.rsqrt(jnp.mean(c * c, axis=1, keepdims=True) + EPS)
            NRM[r, :] = (c * rs * GV[0:1, :] + GV[1:2, :]).astype(bf16)
            STATS[r, 0:1] = mean
            STATS[r, 1:2] = rs

        loop(TILE // unit, norm, UN)
        rows = ds(m * TILE, TILE)
        for i in range(3):
            QKV[i, rows, :] = nn(NRM[rows, :], W[i]).astype(bf16)

    cp_w.wait()
    loop(tiles, p1)

    cp_owr.wait()
    relay = OW.at[ds((1 - hd) * DL + core * half, half, 16), :]
    cp_owc = rt.remote(relay, relay, rt.across(1))
    cp_owc.start()

    low = lax.broadcasted_iota(i32, (CPAD, 128), 1) < HDIM

    def split(v):
        zero = jnp.zeros_like(v)
        return jnp.concatenate([jnp.where(low, v, zero), jnp.where(low, zero, v)], axis=0)

    def fold(v):
        return jnp.where(low, v[:CPAD], v[CPAD:])

    def members(h, p):
        unit = 16
        for a in range(2):
            k = 2 * p + a

            def fill(i):
                row = IDE[h, k : k + 1, :]
                c = lax.broadcasted_iota(i32, (unit, T), 0) + i * unit
                MB[ds(a * CPAD + i * unit, unit), :] = jnp.where(row == c, 1.0, 0.0).astype(bf16)

            loop(CPAD // unit, fill, UA)

    def columns(cols, p):
        lane = lax.broadcasted_iota(i32, (TILE, CPAD), 1)
        parts = []
        for a in range(2):
            k = 2 * p + a
            parts.append(jnp.where(cols[:, k : k + 1] == lane, 1.0, 0.0).astype(bf16))
        return jnp.concatenate(parts, axis=1)

    def own_ids(rows):
        return jnp.where(hd == 0, IDT[rows, 0:8], IDT[rows, 8:16])

    def masked_scores(p, r):
        seg = IDE[hd, 6:7, :].astype(f32)
        allowed = jnp.abs(AUX[p, r, 1:2] - seg) < 0.5
        return jnp.where(allowed, SB[r, :] * SCALE, FAR)

    co_sent = []
    for p in range(NP):
        lanes = pl.ds(p * 128, 128)
        members(hd, p)
        unit = 16

        def count(i):
            r = ds(i * unit, unit)
            v = MB[r, :].astype(f32)
            n = jnp.maximum(jnp.sum(v, axis=1, keepdims=True), 1.0)
            seg = IDE[hd, 6:7, :].astype(f32)
            AUX[p, r, 0:1] = 1.0 / n
            AUX[p, r, 1:2] = jnp.sum(v * seg, axis=1, keepdims=True) / n

        loop(2 * CPAD // unit, count, UA)
        cen = (nn(MB[...], QKV[0, :, lanes]) * AUX[p, :, 0:1]).astype(bf16)
        CEN[p] = split(fold(cen))
        SB[...] = nt(CEN[p], QKV[1, :, lanes])

        def soft(i):
            r = ds(i * unit, unit)
            v = masked_scores(p, r)
            top = jnp.max(v, axis=1, keepdims=True)
            e = jnp.exp(v - top)
            den = jnp.sum(e, axis=1, keepdims=True)
            WB[r, :] = (e * (1.0 / den)).astype(bf16)
            AUX[p, r, 2:3] = top + jnp.log(den)

        loop(2 * CPAD // unit, soft, UA)
        CO[hd * NP + p] = fold(nn(WB[...], QKV[2, :, lanes]).astype(bf16))
        there = CO.at[hd * NP + p]
        copy = rt.remote(there, there, rt.beside)
        copy.start()
        co_sent.append(copy)

    for m in range(tiles):
        og_remote(m).start()

    cp_ow.wait()
    cp_owc.wait()
    for copy in co_sent:
        copy.wait()

    def p3(m):
        rows = ds(m * TILE, TILE)
        for q in range(2 * NP):
            h, p = q // NP, q % NP
            MIX[rows, q * 128 : (q + 1) * 128] = nn(columns(IDT[rows, h * 8 : h * 8 + 8], p), split(CO[q])).astype(bf16)
        PB[...] = nn(MIX[rows, :], OW[...])
        unit = 32

        def norm(i):
            r = ds(m * TILE + i * unit, unit)
            v = X[r, :].astype(f32) + PB[ds(i * unit, unit), :]
            RES[r, :] = v
            mean = jnp.mean(v, axis=1, keepdims=True)
            c = v - mean
            rs = lax.rsqrt(jnp.mean(c * c, axis=1, keepdims=True) + EPS)
            SEC[r, :] = (c * rs * GV[2:3, :] + GV[3:4, :]).astype(bf16)
            STATS[r, 2:3] = mean
            STATS[r, 3:4] = rs

        loop(TILE // unit, norm, UN)

    loop(tiles, p3)

    cp_up.wait()
    cp_dn.wait()
    og_local().wait()
    S2, S2S, S2R, STS, STR = (s[n] for n in ("S2", "S2S", "S2R", "STS", "STR"))
    k_s2, k_st = rt.take(tiles), rt.take(tiles)

    def s2_remote(m):
        rows = ds(m * TILE, TILE)
        return rt.remote(S2S.at[rows, :], S2R.at[rows, :], rt.beside, sem=k_s2 + m)

    def st_remote(m):
        return rt.remote(STS.at[m], STR.at[m], rt.beside, sem=k_st + m)

    def row_sums(m, own, send, out, gain, src, k):
        unit = 32

        def split_rows(i):
            r = ds(m * TILE + i * unit, unit)
            b = ds(i * unit, unit)
            own[r, :] = PB[b, mine]
            send[r, :] = PB[b, away].astype(bf16)
            e = PB[b, :] * GV[gain : gain + 1, :]
            nh = (src[r, :].astype(f32) - STATS[r, k : k + 1]) * STATS[r, k + 1 : k + 2]
            SCOL[b, 0:1] = jnp.sum(e, axis=1, keepdims=True)
            SCOL[b, 1:2] = jnp.sum(e * nh, axis=1, keepdims=True)

        loop(TILE // unit, split_rows, UN)
        out[m] = jnp.transpose(SCOL[...])[0:8, :]

    SCOL[...] = jnp.zeros_like(SCOL)

    def p4(m):
        og_remote(m).wait()
        rows = ds(m * TILE, TILE)

        def chunk(n):
            cols = ds(n * CHUNK, CHUNK)
            HB[...] = nn(SEC[rows, :], UP[:, cols])
            AB[...] = nt(OG[rows, :], DN[cols, :])
            unit = 16

            def gelu(i):
                b = ds(i * unit, unit)
                r = ds(m * TILE + i * unit, unit)
                v = HB[b, :]
                v2 = v * v
                t = jnp.tanh(v * (C0 + C1 * v2))
                hf = 0.5 * t + 0.5
                act = v * hf
                slope = hf + act * (1.0 - hf) * (2 * C0 + 6 * C1 * v2)
                ACT[r, cols] = act.astype(bf16)
                HG[r, cols] = (AB[b, :] * slope).astype(bf16)

            loop(TILE // unit, gelu, UG)

        loop(FL // CHUNK, chunk)
        PB[...] = nt(HG[rows, :], UP[...])
        row_sums(m, S2, S2S, STS, 2, RES, 2)
        s2_remote(m).start()
        st_remote(m).start()

    loop(tiles, p4)

    def total(name, rows, cols, order, acc, base=0, sends=None):
        steps = plan(rows, order)
        count = len(steps)
        if sends is None:
            sends = [s[f"{name}S{k}"] for k in range(count)]
        recvs = [s[f"{name}R{k}"] for k in range(count)]
        return Total(rt, rows, cols, order, acc, base, sends, recvs, s[f"{name}O"])

    dg = total("D", FL, D, orders[0], s["DA"])
    ug_sends = [dg.sends[0]] + [s[f"US{k}"] for k in range(1, len(plan(FL, orders[1])))]
    ug = total("U", FL, D, orders[1], s["UA"], sends=ug_sends)

    def grad_half(left, right, first, rows, tall, store):
        def one(j):
            cols = ds(first + j * tall, tall, 128)
            store(ds(j * tall, tall), tn(left[:, cols], right))

        loop(rows // tall, one)

    def to_low(ref):
        def store(r, v):
            ref[r, :] = v.astype(bf16)

        return store

    def to_full(ref):
        def store(r, v):
            ref[r, :] = v

        return store

    grad_half(ACT, OG[...], (1 - core) * (FL // 2), FL // 2, 384, to_low(dg.sends[0]))
    dg.first_sent()
    grad_half(ACT, OG[...], core * (FL // 2), FL // 2, 384, to_full(dg.acc))
    dg.move()
    hg_half = lambda c: HG[:, ds(c * (FL // 2), FL // 2, 128)]
    grad_half(SEC, hg_half(1 - core), 0, D, 384, to_low(ug.sends[0]))
    ug.first_sent()
    grad_half(SEC, hg_half(core), 0, D, 384, to_full(ug.acc))
    ug.move()

    sums = {"D": dg, "U": ug}

    def point(name):
        for one in SCHED.get(name, ""):
            sums[one].move()

    BG, GACC, MG = HG.at[:, pl.ds(3 * DL, DL)], s["GACC"], SEC
    GACC[...] = jnp.zeros_like(GACC)

    def norm_back(m, own, recv, sums, got, gain, src, k, base, write, slot):
        unit = 16
        SCOL[...] = jnp.transpose(
            jnp.concatenate([sums[m] + got[m], jnp.zeros((120, TILE), f32)], axis=0)
        ) * (1.0 / D)

        def rowsback(i):
            r = ds(m * TILE + i * unit, unit)
            b = ds(i * unit, unit)
            e = own[r, :] + recv[r, :].astype(f32)
            nh = (src[r, mine].astype(f32) - STATS[r, k : k + 1]) * STATS[r, k + 1 : k + 2]
            grad = STATS[r, k + 1 : k + 2] * (
                e * GV[gain : gain + 1, mine] - SCOL[b, 0:1] - nh * SCOL[b, 1:2]
            )
            write(r, base(r) + grad)
            en = e * nh
            GACC[slot] += en[0:8] + en[8:16]
            GACC[slot + 1] += e[0:8] + e[8:16]

        loop(TILE // unit, rowsback, UN)

    def p5(m):
        s2_remote(m).wait()
        st_remote(m).wait()

        def write(r, v):
            S2[r, :] = v
            BG[r, :] = v.astype(bf16)

        norm_back(m, S2, S2R, STS, STR, 2, RES, 2, lambda r: OG[r, mine].astype(f32), write, 2)
        rows = ds(m * TILE, TILE)
        MG[rows, :] = nt(BG[rows, :], OW[:, mine]).astype(bf16)

    loop(tiles, p5)

    CGS, CGR, CGO = s["CGS"], s["CGR"], s["CGO"]

    def reduce_pair(h, p):
        members(h, p)
        lanes = ds((h * NP + p) * 128, 128)
        return fold(nn(MB[...], MG[:, lanes]))

    for p in range(NP):
        CGS[p] = reduce_pair(1 - hd, p).astype(bf16)
    cp_cg = rt.remote(CGS, CGR, rt.beside)
    cp_cg.start()

    MA, MXS, MXR = s["MA"], MIX.at[pl.ds(0, DL), away], s["MXR"]
    MXS[...] = tn(MIX[:, away], BG[...]).astype(bf16)
    cp_mx = rt.remote(MXS, MXR, rt.beside)
    cp_mx.start()
    for p in range(NP):
        CGO[p] = reduce_pair(hd, p)
    MA[ds(hd * DL, DL, 16), :] = tn(MIX[:, mine], BG[...])

    point("r")

    FFS, FFR = MIX.at[:, mine], s["FFR"]
    k_ff = rt.take(tiles)

    def ff_remote(m):
        rows = ds(m * TILE, TILE)
        return rt.remote(FFS.at[rows, :], FFR.at[rows, :], rt.beside, sem=k_ff + m)

    def p6(m):
        rows = ds(m * TILE, TILE)
        PB[...] = nn(ACT[rows, :], DN[...])
        unit = 32

        def split_rows(i):
            r = ds(m * TILE + i * unit, unit)
            b = ds(i * unit, unit)
            RES[r, mine] += PB[b, mine]
            FFS[r, :] = PB[b, away].astype(bf16)

        loop(TILE // unit, split_rows, UN)

    loop(tiles, p6)
    for m in range(tiles // 2):
        ff_remote(m).start()
    point("f")

    PG = HG
    cp_cg.wait()
    for p in range(NP):
        lanes = pl.ds(p * 128, 128)
        cog = split((CGO[p] + CGR[p].astype(f32)).astype(bf16))
        SB[...] = nt(CEN[p], QKV[1, :, lanes])
        DB[...] = nt(cog, QKV[2, :, lanes])
        unit = 16

        def back(i):
            r = ds(i * unit, unit)
            pr = jnp.exp(masked_scores(p, r) - AUX[p, r, 2:3])
            WB[r, :] = pr.astype(bf16)
            dp = DB[r, :]
            dot = jnp.sum(dp * pr, axis=1, keepdims=True)
            MB[r, :] = (pr * (dp - dot)).astype(bf16)

        loop(2 * CPAD // unit, back, 8)
        cg = (nn(MB[...], QKV[1, :, lanes]) * (SCALE * AUX[p, :, 0:1])).astype(bf16)
        cg = split(fold(cg))
        for m in range(tiles):
            rows = pl.ds(m * TILE, TILE)
            at = p * 128
            PG[rows, at : at + 128] = nn(columns(own_ids(rows), p), cg).astype(bf16)
            PG[rows, DL + at : DL + at + 128] = (tn(MB[:, rows], CEN[p]) * SCALE).astype(bf16)
            PG[rows, 2 * DL + at : 2 * DL + at + 128] = tn(WB[:, rows], cog).astype(bf16)
        point(f"b{p}")

    F1, F1S, F1R = RES.at[:, away], S2S, s["F1R"]
    FTS, FTR = s["FTS"], s["FTR"]
    k_f1, k_ft = rt.take(tiles), rt.take(tiles)

    def f1_remote(m):
        rows = ds(m * TILE, TILE)
        return rt.remote(F1S.at[rows, :], F1R.at[rows, :], rt.beside, sem=k_f1 + m)

    def ft_remote(m):
        return rt.remote(FTS.at[m], FTR.at[m], rt.beside, sem=k_ft + m)

    def p8(m):
        rows = ds(m * TILE, TILE)
        acc = nt(PG[rows, 0:DL], W[0])
        acc += nt(PG[rows, DL : 2 * DL], W[1])
        acc += nt(PG[rows, 2 * DL : 3 * DL], W[2])
        PB[...] = acc
        row_sums(m, F1, F1S, FTS, 0, X, 0)
        f1_remote(m).start()
        ft_remote(m).start()

    loop(tiles, p8)
    for m in range(tiles // 2, tiles):
        ff_remote(m).start()
    point("o")

    def act_sends(rows, order, block):
        sends, at = [], 0
        for step, count, halve in plan(rows, order):
            sends.append(ACT.at[pl.ds(at, count), pl.ds(block * DL, DL)])
            at += count
        return sends

    while dg.pos < len(dg.steps):
        dg.move()
    grads = []
    for i in (2, 1, 0):
        name = "QKV"[i]
        room = s["DA"].at[pl.ds(i // 2 * (D // 2), D // 2), pl.ds(i % 2 * DL, DL)]
        tot = total(name, D, DL, orders[2 + i], room, 0, act_sends(D, orders[2 + i], i))
        right = PG[:, i * DL : (i + 1) * DL]
        grad_half(NRM, right, (1 - core) * (D // 2), D // 2, 384, to_low(tot.sends[0]))
        tot.first_sent()
        grad_half(NRM, right, core * (D // 2), D // 2, 384, to_full(tot.acc))
        grads.append(tot)
        sums[name] = tot
        point("qkv"[i])
    vg, kg, qg = grads
    cp_mx.wait()
    mg = total("M", D, DL, orders[5], MA, core * DL, act_sends(D, orders[5], 3))

    def spread(i):
        MA[ds((1 - hd) * DL + i * 16, 16), :] = MXR[ds(i * 16, 16), :].astype(f32)

    loop(DL // 16, spread)

    def mix_half(i):
        mg.sends[0][ds(i * 16, 16), :] = MA[ds((1 - core) * DL + i * 16, 16), :].astype(bf16)

    loop(DL // 16, mix_half)
    mg.first_sent()
    sums["M"] = mg
    point("m")

    LO, IG = S2R, BG

    def p9(m):
        ff_remote(m).wait()
        unit = 32

        def rows_out(i):
            r = ds(m * TILE + i * unit, unit)
            LO[r, :] = (RES[r, mine] + FFR[r, :].astype(f32)).astype(bf16)

        loop(TILE // unit, rows_out, UN)

    loop(tiles, p9)
    cp_lo = rt.local(LO, lo_out)
    cp_lo.start()
    point("l")

    def p10(m):
        f1_remote(m).wait()
        ft_remote(m).wait()

        def write(r, v):
            IG[r, :] = v.astype(bf16)

        norm_back(m, F1, F1R, FTS, FTR, 0, X, 0, lambda r: S2[r, :], write, 0)

    loop(tiles, p10)
    cp_ig = rt.local(IG, ig_out)
    cp_ig.start()
    point("e")

    GX, GR, GO = s["GX"], s["GR"], s["GO"]
    for k in range(4):
        GX[0, k : k + 1, :] = jnp.sum(GACC[k], axis=0, keepdims=True)
    GX[0, 4:8, :] = jnp.zeros((4, DL), f32)
    done = [cp_lo, cp_ig]

    def finish(tot, src, dst):
        copy = rt.local(src, dst)
        copy.start()
        done.append(copy)

    totals = [
        (dg, lambda: finish(dg, s["DO"], d_out)),
        (ug, lambda: [finish(ug, s["UO"].at[pl.ds(j * D, D), :], u_out.at[:, pl.ds(j * D, D)]) for j in range(2)]),
        (vg, lambda: finish(vg, s["VO"], q_out.at[2])),
        (kg, lambda: finish(kg, s["KO"], q_out.at[1])),
        (qg, lambda: finish(qg, s["QO"], q_out.at[0])),
        (mg, lambda: [finish(mg, s["MO"].at[pl.ds(j * DL, DL), :], m_out.at[:, pl.ds(j * DL, DL)]) for j in range(2)]),
    ]
    gain_copy = None
    gain_step = 0

    def gain_move():
        nonlocal gain_copy, gain_step
        if gain_step > nbits + 1:
            return
        if gain_copy is not None:
            gain_copy.wait()
            if gain_step <= nbits:
                GX[gain_step] = GX[gain_step - 1] + GR[gain_step - 1]
            else:
                GO[:, away] = GR[nbits]
                GO[:, mine] = GX[nbits]
                copy = rt.local(GO, g_out)
                copy.start()
                done.append(copy)
        if gain_step < nbits:
            gain_copy = rt.remote(GX.at[gain_step], GR.at[gain_step], rt.across(1 << gain_step))
            gain_copy.start()
        elif gain_step == nbits:
            gain_copy = rt.remote(GX.at[nbits], GR.at[nbits], rt.beside)
            gain_copy.start()
        gain_step += 1

    gain_move()
    while any(tot.left for tot, _ in totals):
        for tot, end in totals:
            if tot.left:
                tot.move()
                if not tot.left:
                    end()
        gain_move()
    while gain_step <= nbits + 1:
        gain_move()
    for copy in done:
        copy.wait()


def layer(nbits, args):
    x, og, w, ow, up, dn, ids, gv = args
    T, DL = x.shape
    D, FL = up.shape
    NP = DL // 128
    bits = [1 << k for k in range(nbits)]
    order_a = list(bits)
    order_b = [bits[0]] + ([bits[2], bits[1]] + bits[3:] if nbits > 2 else bits[1:])
    orders = [order_a, order_b, order_a, order_b, order_a, order_b]
    tiles = T // TILE
    V = pltpu.VMEM
    scratch = [
        ("X", V((T, D), bf16)),
        ("OG", V((T, D), bf16)),
        ("NRM", V((T, D), bf16)),
        ("QKV", V((3, T, DL), bf16)),
        ("W", V((3, D, DL), bf16)),
        ("OW", V((D, D), bf16)),
        ("UP", V((D, FL), bf16)),
        ("DN", V((FL, D), bf16)),
        ("IDS", V((2, 8, T), i32)),
        ("IDE", V((2, 8, T), i32)),
        ("IDT", V((T, 16), i32)),
        ("GV", V((4, D), f32)),
        ("STATS", V((T, 8), f32)),
        ("AUX", V((NP, 2 * CPAD, 8), f32)),
        ("MIX", V((T, D), bf16)),
        ("RES", V((T, D), f32)),
        ("SEC", V((T, D), bf16)),
        ("ACT", V((T, FL), bf16)),
        ("HG", V((T, FL), bf16)),
        ("MB", V((2 * CPAD, T), bf16)),
        ("SB", V((2 * CPAD, T), f32)),
        ("DB", V((2 * CPAD, T), f32)),
        ("WB", V((2 * CPAD, T), bf16)),
        ("CEN", V((NP, 2 * CPAD, 128), bf16)),
        ("CO", V((2 * NP, CPAD, 128), bf16)),
        ("SCOL", V((TILE, 128), f32)),
        ("S2", V((T, DL), f32)),
        ("S2S", V((T, DL), bf16)),
        ("S2R", V((T, DL), bf16)),
        ("STS", V((tiles, 8, TILE), f32)),
        ("STR", V((tiles, 8, TILE), f32)),
        ("GACC", V((4, 8, DL), f32)),
        ("CGS", V((NP, CPAD, 128), bf16)),
        ("CGR", V((NP, CPAD, 128), bf16)),
        ("CGO", V((NP, CPAD, 128), f32)),
        ("MA", V((D, DL), f32)),
        ("MXR", V((DL, DL), bf16)),
        ("FFR", V((T, DL), bf16)),
        ("F1R", V((T, DL), bf16)),
        ("FTS", V((tiles, 8, TILE), f32)),
        ("FTR", V((tiles, 8, TILE), f32)),
        ("GX", V((nbits + 1, 8, DL), f32)),
        ("GR", V((nbits + 1, 8, DL), f32)),
        ("GO", V((8, D), f32)),
        ("DA", V((FL // 2, D), f32)),
        ("UA", V((D, FL // 2), f32)),
    ]
    for name, rows, cols, order, own in (
        ("D", FL, D, orders[0], True),
        ("U", FL, D, orders[1], True),
        ("Q", D, DL, orders[2], False),
        ("K", D, DL, orders[3], False),
        ("V", D, DL, orders[4], False),
        ("M", D, DL, orders[5], False),
    ):
        for k, (step, count, halve) in enumerate(plan(rows, order)):
            if own and (name, k) != ("U", 0):
                scratch.append((f"{name}S{k}", V((count, cols), bf16)))
            scratch.append((f"{name}R{k}", V((count, cols), bf16)))
        scratch.append((f"{name}O", V((rows, cols), bf16)))
    copies = 6 * tiles + 16 + NP + 12 * nbits + nbits
    scratch += [
        ("send_sem", pltpu.SemaphoreType.DMA((copies,))),
        ("recv_sem", pltpu.SemaphoreType.DMA((copies,))),
        ("local_sem", pltpu.SemaphoreType.DMA((tiles + 24,))),
    ]
    shape = jax.ShapeDtypeStruct
    hbm = pl.BlockSpec(memory_space=pl.ANY)
    return pl.pallas_call(
        functools.partial(layer_kernel, [n for n, _ in scratch], nbits, orders),
        out_shape=(
            shape((T, DL), bf16),
            shape((T, DL), bf16),
            shape((3, D, DL), bf16),
            shape((DL, D), bf16),
            shape((D, FL), bf16),
            shape((FL, D), bf16),
            shape((8, D), f32),
        ),
        in_specs=[hbm] * 8,
        out_specs=(hbm,) * 7,
        scratch_shapes=[v for _, v in scratch],
        compiler_params=pltpu.CompilerParams(
            collective_id=0, has_side_effects=True, vmem_limit_bytes=67043328
        ),
        name="layer",
    )(x, og, w, ow, up, dn, ids, gv)


def shards(
    nbits,
    layer_input,
    first_gain,
    first_shift,
    qkv_weight,
    out_weight,
    second_gain,
    second_shift,
    up_weight,
    down_weight,
    segment_ids,
    pad_mask,
    cluster_ids,
    output_grad,
):
    ids = jnp.concatenate([cluster_ids, segment_ids[None], pad_mask[None]], axis=0)
    gains = jnp.stack([first_gain, first_shift, second_gain, second_shift])
    lo, ig, q, m, u, d, g = layer(
        nbits,
        (layer_input, output_grad, qkv_weight, out_weight, up_weight, down_weight, ids, gains),
    )
    return (lo, ig, q.astype(f32), m.astype(f32), u.astype(f32), d.astype(f32), g[0], g[1], g[2], g[3])


def solution(mesh):
    nbits = mesh.shape["dp"].bit_length() - 1
    placed = (
        P("dp", "head"),
        P(),
        P(),
        P(None, None, "head"),
        P("head", None),
        P(),
        P(),
        P(None, "head"),
        P("head", None),
        P("dp"),
        P("dp"),
        P("head", "dp"),
        P("dp", "head"),
    )
    return jax.shard_map(
        functools.partial(shards, nbits),
        mesh=mesh,
        in_specs=placed,
        out_specs=(
            P("dp", "head"),
            P("dp", "head"),
            P(None, None, "head"),
            P("head", None),
            P(None, "head"),
            P("head", None),
            P(),
            P(),
            P(),
            P(),
        ),
        check_vma=False,
    )
```
